128 devices in a mesh: section: 8 (over x, core), ep: 16 (over y, z).
Axes of the slice: x: 4, y: 4, z: 4, core: 2. Of those that a mesh axis runs over, the one named last changes fastest.
Arguments:
- output_grad: bfloat16 [8, 4096, 1024], P('section', 'ep'), may hold values from -6 to 6
- layer_input: bfloat16 [8, 4096, 1024], P('section', 'ep'), may hold values from -6 to 6
- expert_ids: int32 [8, 4096, 8], P('section', 'ep'), may hold values from 0 to 63, all different within a row; in each aligned block of 256 rows (0 to 255, 256 to 511, ..., all dimensions but the last counted through in order) at most 40 rows name the same one
- route_probs: bfloat16 [8, 4096, 8], P('section', 'ep'), may hold values from 0.049804688 to 0.44921875
- gate_weight: bfloat16 [8, 64, 1024, 384], P('section', 'ep'), may hold values from -0.1875 to 0.1875
- up_weight: bfloat16 [8, 64, 1024, 384], P('section', 'ep'), may hold values from -0.1875 to 0.1875
- down_weight: bfloat16 [8, 64, 384, 1024], P('section', 'ep'), may hold values from -0.3125 to 0.3125
- saved_inputs: bfloat16 [8, 64, 640, 1024], P('section', 'ep'), may hold values from -6 to 6
- saved_gate_grad: bfloat16 [8, 64, 640, 384], P('section', 'ep'), may hold values from -0.5 to 0.5
- saved_up_grad: bfloat16 [8, 64, 640, 384], P('section', 'ep'), may hold values from -0.5 to 0.5
- saved_counts: int32 [8, 64, 16], P('section', 'ep'), may hold values from 0 to 40, as said below
Outputs:
- upstream_grad: bfloat16 [8, 4096, 1024], P('section', 'ep')
- prob_grad: bfloat16 [8, 4096, 8], P('section', 'ep')
- gate_weight_grad: bfloat16 [8, 64, 1024, 384], P('section', 'ep')
- up_weight_grad: bfloat16 [8, 64, 1024, 384], P('section', 'ep')
The draws below stay inside these ranges and needn't reach their ends.
Inputs may be any that keep to these rules, and one draw needn't show every extreme that they name: `expert_ids`: each token names 8 different experts. Among the tokens of one device (aligned blocks of 256 tokens of a section) no expert is named more than 40 times, a bound that some block reaches. `saved_counts`: rows of a block at or beyond its count are padding; some block is full in every draw.
All inputs are finite; a program needn't handle non-finite values.
Results may differ from the reference program's by a relative error of at most 0.008.
Values may be sent and summed in bfloat16 or wider, within the bound.
No kernel may reach another device: no remote copies, remote signals or barrier semaphores. Data moves between devices by JAX's collectives and lax.ppermute only.
A program may use at most 128 MiB of HBM per device.

```python
import math
import jax
import jax.numpy as jnp
import numpy as np
from jax import lax

D = 1024
FF = 384
TOP = 8
TOK_DEV = 256
SECTIONS = 8
TOKENS = 4096
EXPERTS = 64
SOURCES = 16
CAP = 40
SLOTS = 640
N_EP = 16


def draw_saved_counts(key, part):
    base = jax.random.randint(jax.random.fold_in(key, 11), (SECTIONS, EXPERTS, SOURCES), 0, CAP + 1)
    chosen = jax.random.randint(jax.random.fold_in(key, 12), (SECTIONS, 1, 1), 0, EXPERTS * SOURCES)
    flat = jnp.arange(EXPERTS * SOURCES, dtype=jnp.int32).reshape(1, EXPERTS, SOURCES)
    return jnp.where(flat == chosen, CAP, base).astype(jnp.int32)


def block_scale(rng, shape, shards, least, high):
    factor_of, own = 1.0, jax.random.fold_in(rng, 6)
    for axis_at, blocks in shards:
        draws = jnp.exp(jax.random.uniform(jax.random.fold_in(own, axis_at), (blocks,), jnp.float32, least / len(shards), high / len(shards)))
        factor_of = factor_of * jnp.repeat(draws, shape[axis_at] // blocks).reshape([-1 if axis == axis_at else 1 for axis in range(len(shape))])
    return factor_of


def deal_out(key, own, number, rows, amount, top, reach, slope):
    sequence = jax.random.permutation(key, amount)
    packed, common = shares(amount, rows * top, reach, slope, True), shares(amount, rows * top, reach, slope, False)
    places = jnp.arange(amount)

    def named(sizes, rotation):
        used = int((sizes > 0).sum())
        fixed = max(1, used // 4)
        passed = fixed + (places - fixed + rotation * (used - fixed)) % max(1, amount - fixed)
        return jnp.zeros((amount,), jnp.int32).at[sequence[jnp.where(places < fixed, places, passed)]].set(jnp.asarray(sizes, jnp.int32))

    sizes = jnp.where(number % 4 == 0, named(packed, number // 4), named(common, number - number // 4 - 1))
    mixed = jax.random.permutation(jax.random.fold_in(own, 3), amount)
    giver, receiver = mixed[0:amount // 2 * 2:2], mixed[1:amount // 2 * 2:2]
    slack = jnp.minimum(sizes[giver] - 1, reach - sizes[receiver]) // 2
    slack = jnp.where((giver == sequence[0]) | (receiver == sequence[0]) | (sizes[receiver] == 0), 0, jnp.maximum(slack, 0))
    passed = jax.random.randint(jax.random.fold_in(own, 4), (amount // 2,), 0, 1 << 20) % (slack + 1)
    sizes = sizes.at[giver].add(-passed).at[receiver].add(passed)
    labels = jnp.searchsorted(jnp.cumsum(sizes), jnp.arange(rows * top), side="right").astype(jnp.int32)
    grid = labels.reshape(top, rows).T
    grid = grid[jax.random.permutation(jax.random.fold_in(own, 1), rows)]
    rotation = jax.random.randint(jax.random.fold_in(own, 2), (rows, 1), 0, top)
    return jnp.take_along_axis(grid, (jnp.arange(top)[None, :] + rotation) % top, axis=1)


def shares(amount, total, limit, skew, full):
    weights = [(1 << 20) // math.isqrt(rank ** skew) + 1 for rank in range(1, amount + 1)]
    largest = limit if full else min(limit, max(-(-total // amount), total * weights[0] // sum(weights)))
    least = 1 if total - largest >= amount - 1 else 0
    given, spare = [largest] + [least] * (amount - 1), total - largest - least * (amount - 1)
    while spare > 0:
        free = [i for i in range(1, amount) if given[i] < largest] or [i for i in range(1, amount) if given[i] < limit]
        whole, budget = sum([weights[i] for i in free]), spare
        for i in free:
            more = min(limit - given[i], max(1, budget * weights[i] // whole), spare)
            given[i] = given[i] + more
            spare = spare - more
    return np.array(given)


def scatter_about(key, shape, deviation, reach, pieces=(), held_as=jnp.bfloat16):
    values = jax.random.normal(key, shape, jnp.float32) * deviation
    if len(pieces) > 0:
        values = block_scale(key, shape, pieces, -0.22, 0.18) * values
    return jnp.clip(values, min=-reach, max=reach).astype(held_as)


def setup_inputs(seed: int = 0) -> dict:
    splits = jax.random.split(jax.random.key(seed), 12)
    output_grad = scatter_about(splits[0], (SECTIONS, TOKENS, D), 1.0, 6.0, ((0, 8), (1, 16)))
    layer_input = scatter_about(splits[1], (SECTIONS, TOKENS, D), 1.0, 6.0, ((0, 8), (1, 16)))
    expert_ids_keys = jax.random.split(jax.random.fold_in(splits[2], 1), SECTIONS * TOKENS // TOK_DEV)
    expert_ids_turns = jax.random.permutation(jax.random.fold_in(splits[2], 3), SECTIONS * TOKENS // TOK_DEV)
    expert_ids = jax.vmap(lambda own, number: deal_out(jax.random.fold_in(splits[2], 2), own, number, TOK_DEV, EXPERTS, TOP, CAP, 2))(expert_ids_keys, expert_ids_turns).reshape((SECTIONS, TOKENS, TOP))
    route_probs = jnp.clip(0.049804688 + 0.39941406 * jax.random.uniform(splits[3], (SECTIONS, TOKENS, TOP), jnp.float32) ** block_scale(splits[3], (SECTIONS, TOKENS, TOP), ((0, 8), (1, 16)), -0.2, 0.2), 0.049804688, 0.44921875).astype(jnp.bfloat16)
    gate_weight = scatter_about(splits[4], (SECTIONS, EXPERTS, D, FF), D ** -0.5, 0.1875, ((0, 8), (1, 16)))
    up_weight = scatter_about(splits[5], (SECTIONS, EXPERTS, D, FF), D ** -0.5, 0.1875, ((0, 8), (1, 16)))
    down_weight = scatter_about(splits[6], (SECTIONS, EXPERTS, FF, D), FF ** -0.5, 0.3125, ((0, 8), (1, 16)))
    saved_inputs = scatter_about(splits[7], (SECTIONS, EXPERTS, SLOTS, D), 1.0, 6.0, ((0, 8), (1, 16)))
    saved_gate_grad = scatter_about(splits[8], (SECTIONS, EXPERTS, SLOTS, FF), 0.0625, 0.5, ((0, 8), (1, 16)))
    saved_up_grad = scatter_about(splits[9], (SECTIONS, EXPERTS, SLOTS, FF), 0.0625, 0.5, ((0, 8), (1, 16)))
    saved_counts = draw_saved_counts(jax.random.fold_in(splits[11], 71), 0)
    return {"output_grad": output_grad, "layer_input": layer_input, "expert_ids": expert_ids, "route_probs": route_probs, "gate_weight": gate_weight, "up_weight": up_weight, "down_weight": down_weight, "saved_inputs": saved_inputs, "saved_gate_grad": saved_gate_grad, "saved_up_grad": saved_up_grad, "saved_counts": saved_counts}


def block_slots(block_ids):
    flat_ids = block_ids.reshape(-1)
    onehot = (flat_ids[:, None] == jnp.arange(EXPERTS, dtype=jnp.int32)[None, :]).astype(jnp.int32)
    before = jnp.cumsum(onehot, axis=0) - onehot
    return jnp.sum(before * onehot, axis=1).astype(jnp.int32)


def expert_backward(operands):
    grad_rows, input_rows, prob_rows, w_gate, w_up, w_down = operands
    gate_pre = jnp.dot(input_rows, w_gate, preferred_element_type=jnp.float32)
    up_pre = jnp.dot(input_rows, w_up, preferred_element_type=jnp.float32)
    sigma = jax.nn.sigmoid(gate_pre)
    active = gate_pre * sigma
    hidden = (active * up_pre).astype(jnp.bfloat16)
    hidden_grad = jnp.dot(grad_rows, w_down.T, preferred_element_type=jnp.float32)
    output_rows = jnp.dot(hidden, w_down, preferred_element_type=jnp.float32)
    slot_prob = jnp.sum(output_rows * grad_rows.astype(jnp.float32), axis=1).astype(jnp.bfloat16)
    scaled = hidden_grad * prob_rows.astype(jnp.float32)[:, None]
    gate_grad = (scaled * up_pre * sigma * (1.0 + gate_pre * (1.0 - sigma))).astype(jnp.bfloat16)
    up_grad = (scaled * active).astype(jnp.bfloat16)
    slot_grad = jnp.dot(gate_grad, w_gate.T, preferred_element_type=jnp.float32)
    slot_grad = slot_grad + jnp.dot(up_grad, w_up.T, preferred_element_type=jnp.float32)
    return slot_grad.astype(jnp.bfloat16), slot_prob


def weight_pair(operands):
    masked, gate_grad, up_grad = operands
    gate_part = jnp.dot(masked.T, gate_grad, preferred_element_type=jnp.float32).astype(jnp.bfloat16)
    up_part = jnp.dot(masked.T, up_grad, preferred_element_type=jnp.float32).astype(jnp.bfloat16)
    return gate_part, up_part


def section_pass(grad, inputs, ids, probs, w_gate, w_up, w_down):
    blocks = ids.reshape(N_EP, TOK_DEV * TOP)
    slots = jax.vmap(block_slots)(blocks)
    source = jnp.arange(N_EP, dtype=jnp.int32)[:, None]
    place = (blocks * SLOTS + source * CAP + slots).reshape(-1).astype(jnp.int32)
    token = (jnp.arange(TOKENS * TOP, dtype=jnp.int32) // TOP).astype(jnp.int32)
    grad_rows = jnp.zeros((EXPERTS * SLOTS, D), jnp.bfloat16).at[place].set(grad[token])
    input_rows = jnp.zeros((EXPERTS * SLOTS, D), jnp.bfloat16).at[place].set(inputs[token])
    prob_rows = jnp.zeros((EXPERTS * SLOTS,), jnp.bfloat16).at[place].set(probs.reshape(-1))
    slot_grad, slot_prob = lax.map(expert_backward, (grad_rows.reshape(EXPERTS, SLOTS, D), input_rows.reshape(EXPERTS, SLOTS, D), prob_rows.reshape(EXPERTS, SLOTS), w_gate, w_up, w_down))
    picked = slot_grad.reshape(EXPERTS * SLOTS, D)[place]
    input_grad = jnp.sum(picked.reshape(TOKENS, TOP, D).astype(jnp.float32), axis=1).astype(jnp.bfloat16)
    prob_part = slot_prob.reshape(-1)[place].reshape(TOKENS, TOP)
    return input_grad, prob_part


def weight_pass(inputs, gate_grad, up_grad, counts):
    capacity = jnp.arange(CAP, dtype=jnp.int32)
    live = (capacity[None, None, :] < counts[:, :, None]).reshape(EXPERTS, SLOTS)
    masked = inputs * live.astype(jnp.bfloat16)[:, :, None]
    return lax.map(weight_pair, (masked, gate_grad, up_grad))


def reference(output_grad, layer_input, expert_ids, route_probs, gate_weight, up_weight, down_weight, saved_inputs, saved_gate_grad, saved_up_grad, saved_counts):
    input_grads = []
    prob_grads = []
    gate_grads = []
    up_grads = []
    for section_index in range(SECTIONS):
        input_grad, prob_part = section_pass(output_grad[section_index], layer_input[section_index], expert_ids[section_index], route_probs[section_index], gate_weight[section_index], up_weight[section_index], down_weight[section_index])
        gate_part, up_part = weight_pass(saved_inputs[section_index], saved_gate_grad[section_index], saved_up_grad[section_index], saved_counts[section_index])
        input_grads.append(input_grad)
        prob_grads.append(prob_part)
        gate_grads.append(gate_part)
        up_grads.append(up_part)
    stacked = jnp.stack(input_grads)
    upstream_grad = jnp.concatenate([stacked[1:], jnp.zeros_like(stacked[:1])], axis=0)
    return upstream_grad, jnp.stack(prob_grads), jnp.stack(gate_grads), jnp.stack(up_grads)
```

```python
import functools

import jax
import jax.numpy as jnp
from jax import lax
from jax.experimental import pallas as pl
from jax.experimental.pallas import tpu as pltpu
from jax.sharding import PartitionSpec as P

BF = jnp.bfloat16
F32 = jnp.float32
SIDE = 4
CAP = 40


def along_z(k):
    return [(4 * y + z, 4 * y + (z + k) % 4) for y in range(4) for z in range(4)]


def along_y(k):
    return [(4 * y + z, 4 * ((y + k) % 4) + z) for y in range(4) for z in range(4)]


def moved(array, pairs):
    return lax.ppermute(array, "ep", pairs)


def iota(shape, dim):
    return lax.broadcasted_iota(jnp.int32, shape, dim)


def expert_of_row(dest_ref, rows, per_dest, first):
    row = iota((rows, 256), 0)
    expert = jnp.zeros((rows, 256), jnp.int32)
    for i in range(SIDE):
        expert = jnp.where(row // per_dest == i, 4 * dest_ref[i] + first + row % per_dest, expert)
    return expert.astype(F32)


def earlier():
    return (iota((256, 256), 0) < iota((256, 256), 1)).astype(BF)


def select_body(dest_ref, *refs, first):
    blocks, outs = refs[:4], refs[4:]
    expert = expert_of_row(dest_ref, 8, 2, first)
    marks = []
    for block in blocks:
        ids = block[256:264, 0:256].astype(F32)
        mark = jnp.zeros((8, 256), F32)
        for k in range(8):
            mark = mark + jnp.where(ids[k : k + 1, :] == expert, 1.0, 0.0)
        marks.append(mark)
    mark = jnp.concatenate(marks, axis=0)
    rank = jnp.dot(mark.astype(BF), earlier(), preferred_element_type=F32)
    rank = jnp.where(mark > 0.0, rank, -1.0)
    slot = iota((8, CAP, 256), 1).astype(F32)
    for j, block in enumerate(blocks):
        mine = rank[8 * j : 8 * j + 8]
        pick = jnp.where(mine[:, None, :] == slot, 1.0, 0.0).reshape(8 * CAP, 256).astype(BF)
        rows = jnp.dot(pick, block[0:256, :], preferred_element_type=F32)
        for i in range(SIDE):
            for e in range(2):
                at = (2 * i + e) * CAP
                outs[i][e, j] = rows[at : at + CAP].astype(BF)


def select(dest, blocks, first):
    out = jax.ShapeDtypeStruct((2, SIDE, CAP, 1024), BF)
    return pl.pallas_call(
        functools.partial(select_body, first=first),
        out_shape=(out,) * 4,
        grid_spec=pltpu.PrefetchScalarGridSpec(
            num_scalar_prefetch=1,
            grid=(1,),
            in_specs=[pl.BlockSpec((264, 1024), lambda g, d: (0, 0))] * 4,
            out_specs=[pl.BlockSpec((2, SIDE, CAP, 1024), lambda g, d: (0, 0, 0, 0))] * 4,
        ),
        name="select",
    )(dest, *blocks)


def expert_body(*refs, half):
    xs, gs = refs[0:4], refs[4:8]
    wg_ref, wu_ref, wd_ref = refs[8:11]
    before = refs[11:15]
    a_outs, b_outs, p_outs = refs[15:19], refs[19:23], refs[23:27]
    e = pl.program_id(0)
    rows = jnp.concatenate([r[0] for r in xs], axis=0)
    grads = jnp.concatenate([r[0] for r in gs], axis=0)
    wg, wu, wd = wg_ref[0], wu_ref[0], wd_ref[0]
    nt = (((1,), (1,)), ((), ()))
    gate = jnp.dot(rows, wg, preferred_element_type=F32)
    up = jnp.dot(rows, wu, preferred_element_type=F32)
    hg = lax.dot_general(grads, wd, nt, preferred_element_type=F32)
    hg = jnp.concatenate(
        [hg[(4 * j + i) * CAP : (4 * j + i + 1) * CAP] for i in range(4) for j in range(4)], axis=0
    )
    sigma = jax.nn.sigmoid(gate)
    active = gate * sigma
    hidden = (active * up).astype(BF).astype(F32)
    prob = jnp.sum(hidden * hg, axis=1, keepdims=True)
    gate_grad = (hg * up * sigma * (1.0 + gate * (1.0 - sigma))).astype(BF)
    up_grad = (hg * active).astype(BF)
    lane = iota((CAP, 128), 1) - 4 * (2 * half + e)
    for i in range(4):
        mine = jnp.zeros((CAP, 128), F32)
        for j in range(4):
            at = (4 * i + j) * CAP
            mine = jnp.where(lane == j, prob[at : at + CAP], mine)
        old = jnp.where(e == 0, before[i][...].astype(F32), p_outs[i][...].astype(F32))
        fresh = (lane >= 0) & (lane < 4)
        p_outs[i][...] = jnp.where(fresh, mine, old).astype(BF)
    back = lax.dot_general(gate_grad, wg, nt, preferred_element_type=F32)
    back = back + lax.dot_general(up_grad, wu, nt, preferred_element_type=F32)
    for i in range(4):
        for j in range(4):
            at = (4 * i + j) * CAP
            a_outs[i][0, j] = back[at : at + CAP, 0:512].astype(BF)
            b_outs[j][0, i] = back[at : at + CAP, 512:1024].astype(BF)


def experts(xs, gs, w_gate, w_up, w_down, before, half):
    rows = pl.BlockSpec((1, 160, 1024), lambda e: (e, 0, 0))
    w_in = pl.BlockSpec((1, 1024, 384), lambda e: (2 * half + e, 0, 0))
    w_out = pl.BlockSpec((1, 384, 1024), lambda e: (2 * half + e, 0, 0))
    probs = pl.BlockSpec((CAP, 128), lambda e: (0, 0))
    back = pl.BlockSpec((1, SIDE, CAP, 512), lambda e: (e, 0, 0, 0))
    flat = [a.reshape(2, 160, 1024) for a in (*xs, *gs)]
    out = jax.ShapeDtypeStruct((2, SIDE, CAP, 512), BF)
    outs = pl.pallas_call(
        functools.partial(expert_body, half=half),
        out_shape=(out,) * 8 + (jax.ShapeDtypeStruct((CAP, 128), BF),) * 4,
        grid=(2,),
        in_specs=[rows] * 8 + [w_in, w_in, w_out] + [probs] * 4,
        out_specs=[back] * 8 + [probs] * 4,
        compiler_params=pltpu.CompilerParams(vmem_limit_bytes=56 * 1024 * 1024),
        name="experts",
    )(*flat, w_gate, w_up, w_down, *before)
    return outs[0:4], outs[4:8], outs[8:12]


def combine_body(dest_ref, *refs, with_prob):
    metas, low, high = refs[0:4], refs[4:8], refs[8:12]
    probs = refs[12:16] if with_prob else ()
    outs = refs[-4:]
    expert = expert_of_row(dest_ref, 16, 4, 0)
    marks, scales = [], []
    for meta in metas:
        ids = meta[:, 0:256].astype(F32)
        weight = meta[:, 256:512].astype(F32)
        mark = jnp.zeros((16, 256), F32)
        scale = jnp.zeros((16, 256), F32)
        for k in range(8):
            hit = ids[k : k + 1, :] == expert
            mark = mark + jnp.where(hit, 1.0, 0.0)
            scale = scale + jnp.where(hit, weight[k : k + 1, :], 0.0)
        marks.append(mark)
        scales.append(scale)
    mark = jnp.concatenate(marks, axis=0)
    rank = jnp.dot(mark.astype(BF), earlier(), preferred_element_type=F32)
    rank = jnp.where(mark > 0.0, rank, -1.0)
    slot = iota((16, CAP, 256), 1).astype(F32)
    if with_prob:
        columns = [p[...].astype(F32) for p in probs]
    for j in range(4):
        mine = rank[16 * j : 16 * j + 16]
        hit = mine[:, None, :] == slot
        spread = jnp.where(hit, scales[j][:, None, :], 0.0).reshape(16 * CAP, 256)
        pieces = []
        for i in range(4):
            for e in range(4):
                source = low[i] if e < 2 else high[i]
                pieces.append(source[e % 2, j].astype(F32))
        rows = jnp.concatenate(pieces, axis=0).astype(BF)
        total = jnp.dot(spread.T.astype(BF), rows, preferred_element_type=F32)
        outs[j][0:256, :] = total.astype(BF)
        if with_prob:
            found = []
            for i in range(4):
                for e in range(4):
                    at = 4 * e + j
                    one = jnp.where(mine[4 * i + e : 4 * i + e + 1] == slot[0], columns[i][:, at : at + 1], 0.0)
                    found.append(jnp.sum(one, axis=0, keepdims=True))
            outs[j][256:264, 0:256] = jnp.concatenate(found[0:8], axis=0).astype(BF)
            outs[j][256:264, 256:512] = jnp.concatenate(found[8:16], axis=0).astype(BF)


def combine(dest, blocks, low, high, probs):
    with_prob = len(probs) > 0
    height = 264 if with_prob else 256
    rows = pl.BlockSpec((2, SIDE, CAP, 512), lambda g, d: (0, 0, 0, 0))
    return pl.pallas_call(
        functools.partial(combine_body, with_prob=with_prob),
        out_shape=(jax.ShapeDtypeStruct((height, 512), BF),) * 4,
        grid_spec=pltpu.PrefetchScalarGridSpec(
            num_scalar_prefetch=1,
            grid=(1,),
            in_specs=[pl.BlockSpec((8, 1024), lambda g, d: (32, 0))] * 4
            + [rows] * 8
            + [pl.BlockSpec((CAP, 128), lambda g, d: (0, 0))] * len(probs),
            out_specs=[pl.BlockSpec((height, 512), lambda g, d: (0, 0))] * 4,
        ),
        name="combine",
    )(dest, *blocks, *low, *high, *probs)


def finish_body(place_ref, meta, *refs):
    left, right = refs[0:4], refs[4:8]
    out_ref, prob_ref = refs[8], refs[9]
    total = left[0][0:256, :].astype(F32)
    other = right[0][...].astype(F32)
    for j in range(1, 4):
        total = total + left[j][0:256, :].astype(F32)
        other = other + right[j][...].astype(F32)
    out_ref[:, 0:512] = total.astype(BF)
    out_ref[:, 512:1024] = other.astype(BF)
    ids = meta[:, 0:256].astype(F32)
    row = iota((8, 256), 0)
    found = [jnp.zeros((8, 256), F32) for _ in range(8)]
    for j in range(4):
        for part in range(2):
            values = left[j][256:264, 256 * part : 256 * part + 256].astype(F32)
            device = jnp.where(row // 4 == 0, place_ref[4 * j + 2 * part], place_ref[4 * j + 2 * part + 1])
            expert = (4 * device + row % 4).astype(F32)
            for k in range(8):
                found[k] = found[k] + jnp.where(ids[k : k + 1, :] == expert, values, 0.0)
    rows = [jnp.sum(f, axis=0, keepdims=True) for f in found]
    prob_ref[...] = jnp.concatenate(rows, axis=0).astype(BF)


def finish(places, block, left, right):
    return pl.pallas_call(
        finish_body,
        out_shape=(jax.ShapeDtypeStruct((256, 1024), BF), jax.ShapeDtypeStruct((8, 256), BF)),
        grid_spec=pltpu.PrefetchScalarGridSpec(
            num_scalar_prefetch=1,
            grid=(1,),
            in_specs=[pl.BlockSpec((8, 1024), lambda g, d: (32, 0))]
            + [pl.BlockSpec((264, 512), lambda g, d: (0, 0))] * 4
            + [pl.BlockSpec((256, 512), lambda g, d: (0, 0))] * 4,
            out_specs=[
                pl.BlockSpec((256, 1024), lambda g, d: (0, 0)),
                pl.BlockSpec((8, 256), lambda g, d: (0, 0)),
            ],
        ),
        name="finish",
    )(places, block, *left, *right)


def weight_grads(saved_inputs, saved_gate_grad, saved_up_grad, counts):
    local, slots, _ = saved_inputs.shape
    live = jnp.arange(CAP, dtype=jnp.int32)[None, None, :] < counts[:, :, None]
    masked = saved_inputs * live.reshape(local, slots).astype(BF)[:, :, None]
    gate_part = jnp.einsum("esd,esf->edf", masked, saved_gate_grad, preferred_element_type=F32)
    up_part = jnp.einsum("esd,esf->edf", masked, saved_up_grad, preferred_element_type=F32)
    return gate_part.astype(BF), up_part.astype(BF)


def per_device(
    output_grad,
    layer_input,
    expert_ids,
    route_probs,
    gate_weight,
    up_weight,
    down_weight,
    saved_inputs,
    saved_gate_grad,
    saved_up_grad,
    saved_counts,
):
    here = lax.axis_index("ep").astype(jnp.int32)
    y, z = here // 4, here % 4
    steps = jnp.arange(4, dtype=jnp.int32)
    column = 4 * ((y + steps) % 4) + z
    row = 4 * y + (z + steps) % 4
    places = (4 * ((y + steps) % 4)[None, :] + ((z + steps) % 4)[:, None]).reshape(16)
    w_gate, w_up, w_down = gate_weight[0], up_weight[0], down_weight[0]

    meta = jnp.concatenate(
        [expert_ids[0].T.astype(BF), route_probs[0].T, jnp.zeros((8, 512), BF)], axis=1
    )
    block_a = jnp.concatenate([layer_input[0], meta], axis=0)
    block_b = jnp.concatenate([output_grad[0], meta], axis=0)
    blocks_a = [block_a] + [moved(block_a, along_z(j)) for j in (1, 2, 3)]
    blocks_b = [block_b] + [moved(block_b, along_y(j)) for j in (1, 2, 3)]

    gate_part, up_part = weight_grads(
        saved_inputs[0], saved_gate_grad[0], saved_up_grad[0], saved_counts[0]
    )

    probs = [jnp.zeros((CAP, 128), BF)] * 4
    lows, highs = [], []
    for half in range(2):
        sent_a = select(column, blocks_a, 2 * half)
        sent_b = select(row, blocks_b, 2 * half)
        xs = [sent_a[0]] + [moved(sent_a[i], along_y(i)) for i in (1, 2, 3)]
        gs = [sent_b[0]] + [moved(sent_b[i], along_z(i)) for i in (1, 2, 3)]
        back_a, back_b, probs = experts(xs, gs, w_gate, w_up, w_down, probs, half)
        lows.append([back_a[0]] + [moved(back_a[i], along_y(-i)) for i in (1, 2, 3)])
        highs.append([back_b[0]] + [moved(back_b[i], along_z(-i)) for i in (1, 2, 3)])
    probs = [probs[0]] + [moved(probs[i], along_y(-i)) for i in (1, 2, 3)]

    made_a = combine(column, blocks_a, lows[0], lows[1], probs)
    made_b = combine(row, blocks_b, highs[0], highs[1], ())
    left = [made_a[0]] + [moved(made_a[j], along_z(-j)) for j in (1, 2, 3)]
    right = [made_b[0]] + [moved(made_b[j], along_y(-j)) for j in (1, 2, 3)]
    input_grad, prob_rows = finish(places, block_a, left, right)
    sections = lax.axis_size("section")
    upstream = lax.ppermute(input_grad, "section", [(s, s - 1) for s in range(1, sections)])
    return (upstream[None], prob_rows.T[None], gate_part[None], up_part[None])


def solution(mesh):
    rows = P("section", "ep", None)
    stacks = P("section", "ep", None, None)
    return jax.shard_map(
        per_device,
        mesh=mesh,
        in_specs=(rows, rows, rows, rows) + (stacks,) * 6 + (rows,),
        out_specs=(rows, rows, stacks, stacks),
        check_vma=False,
    )
```

```python
import functools

import jax
import jax.numpy as jnp
from jax import lax
from jax.experimental import pallas as pl
from jax.experimental.pallas import tpu as pltpu
from jax.sharding import PartitionSpec as P


BF = jnp.bfloat16
F32 = jnp.float32
SIDE = 4
CAP = 40


def along_z(k):
    return [(4 * y + z, 4 * y + (z + k) % 4) for y in range(4) for z in range(4)]


def along_y(k):
    return [(4 * y + z, 4 * ((y + k) % 4) + z) for y in range(4) for z in range(4)]


def moved(array, pairs):
    return lax.ppermute(array, "ep", pairs)


def iota(shape, dim):
    return lax.broadcasted_iota(jnp.int32, shape, dim)


def expert_of_row(dest_ref, rows, per_dest, first, base):
    row = iota((rows, 256), 0)
    expert = jnp.zeros((rows, 256), jnp.int32)
    for i in range(SIDE):
        expert = jnp.where(row // per_dest == i, 4 * dest_ref[base + i] + first + row % per_dest, expert)
    return expert.astype(F32)


def earlier():
    return (iota((256, 256), 0) < iota((256, 256), 1)).astype(BF)


def slot_ranks(ids_list, expert, rows):
    marks = []
    for ids in ids_list:
        mark = jnp.zeros((rows, 256), F32)
        for k in range(8):
            mark = mark + jnp.where(ids[k : k + 1, :] == expert, 1.0, 0.0)
        marks.append(mark)
    mark = jnp.concatenate(marks, axis=0)
    rank = jnp.dot(mark.astype(BF), earlier(), preferred_element_type=F32)
    rank = jnp.where(mark > 0.0, rank, -1.0)
    return [rank[rows * j : rows * j + rows] for j in range(len(ids_list))]


def select_body(dest_ref, *refs, first):
    blocks, outs = refs[:8], refs[8:16]
    held, stage, in_sems, out_sems = refs[16:]
    order = [4 * c + j for j in range(4) for c in range(2)]
    loads = [pltpu.make_async_copy(blocks[n], held.at[n], in_sems.at[n]) for n in range(8)]
    for n in order:
        loads[n].start()
    experts = [expert_of_row(dest_ref, 8, 2, first, 4 * c) for c in range(2)]
    slot = iota((8, CAP, 256), 1).astype(F32)
    stores = []
    for n in order:
        loads[n].wait()
        c, j = n // 4, n % 4
        mine = slot_ranks([held[n, 256:264, 0:256].astype(F32)], experts[c], 8)[0]
        pick = jnp.where(mine[:, None, :] == slot, 1.0, 0.0).reshape(8 * CAP, 256).astype(BF)
        rows = jnp.dot(pick, held[n, 0:256, :], preferred_element_type=F32)
        for i in range(SIDE):
            for e in range(2):
                at = (2 * i + e) * CAP
                stage[n, i, e] = rows[at : at + CAP].astype(BF)
            store = pltpu.make_async_copy(stage.at[n, i], outs[4 * c + i].at[:, j], out_sems.at[4 * n + i])
            store.start()
            stores.append(store)
    for store in stores:
        store.wait()


def select(dest, blocks_a, blocks_b, first):
    out = jax.ShapeDtypeStruct((2, SIDE, CAP, 1024), BF)
    anywhere = pl.BlockSpec(memory_space=pl.ANY)
    outs = pl.pallas_call(
        functools.partial(select_body, first=first),
        out_shape=(out,) * 8,
        grid_spec=pltpu.PrefetchScalarGridSpec(
            num_scalar_prefetch=1,
            grid=(1,),
            in_specs=[anywhere] * 8,
            out_specs=[anywhere] * 8,
            scratch_shapes=[
                pltpu.VMEM((8, 264, 1024), BF),
                pltpu.VMEM((8, SIDE, 2, CAP, 1024), BF),
                pltpu.SemaphoreType.DMA((8,)),
                pltpu.SemaphoreType.DMA((32,)),
            ],
        ),
        name="select",
    )(dest, *blocks_a, *blocks_b)
    return outs[:4], outs[4:]


def spread_body(dest_ref, *refs):
    metas, outs = refs[:8], refs[8:]
    slot = iota((16, CAP, 256), 1).astype(F32)
    for c in range(2):
        expert = expert_of_row(dest_ref, 16, 4, 0, 4 * c)
        mine = metas[4 * c : 4 * c + 4]
        ids_list = [m[:, 0:256].astype(F32) for m in mine]
        ranks = slot_ranks(ids_list, expert, 16)
        for j in range(4):
            weight = mine[j][:, 256:512].astype(F32)
            scale = jnp.zeros((16, 256), F32)
            for k in range(8):
                scale = scale + jnp.where(ids_list[j][k : k + 1, :] == expert, weight[k : k + 1, :], 0.0)
            spread = jnp.where(ranks[j][:, None, :] == slot, scale[:, None, :], 0.0).reshape(16 * CAP, 256)
            outs[c][j] = spread.T.astype(BF)


def spreads(dest, blocks_a, blocks_b):
    return pl.pallas_call(
        spread_body,
        out_shape=(jax.ShapeDtypeStruct((SIDE, 256, 16 * CAP), BF),) * 2,
        grid_spec=pltpu.PrefetchScalarGridSpec(
            num_scalar_prefetch=1,
            grid=(1,),
            in_specs=[pl.BlockSpec((8, 1024), lambda g, d: (32, 0))] * 8,
            out_specs=[pl.BlockSpec((SIDE, 256, 16 * CAP), lambda g, d: (0, 0, 0))] * 2,
        ),
        name="spreads",
    )(dest, *blocks_a, *blocks_b)


def expert_body(*refs):
    xs, gs = refs[0:4], refs[4:8]
    wg_ref, wu_ref, wd_ref = refs[8:11]
    a_outs, b_outs = refs[-8:-4], refs[-4:]
    rows = jnp.concatenate([r[0] for r in xs], axis=0)
    grads = jnp.concatenate([r[0] for r in gs], axis=0)
    wg, wu, wd = wg_ref[0], wu_ref[0], wd_ref[0]
    nt = (((1,), (1,)), ((), ()))
    gate = jnp.dot(rows, wg, preferred_element_type=F32)
    up = jnp.dot(rows, wu, preferred_element_type=F32)
    hg = lax.dot_general(grads, wd, nt, preferred_element_type=F32)
    hg = jnp.concatenate(
        [hg[(4 * j + i) * CAP : (4 * j + i + 1) * CAP] for i in range(4) for j in range(4)], axis=0
    )
    sigma = jax.nn.sigmoid(gate)
    active = gate * sigma
    hidden = (active * up).astype(BF).astype(F32)
    prob = jnp.sum(hidden * hg, axis=1, keepdims=True)
    gate_grad = (hg * up * sigma * (1.0 + gate * (1.0 - sigma))).astype(BF)
    up_grad = (hg * active).astype(BF)
    lane = iota((CAP, 128), 1)
    for i in range(4):
        mine = jnp.zeros((CAP, 128), F32)
        for j in range(4):
            at = (4 * i + j) * CAP
            mine = jnp.where(lane == j, prob[at : at + CAP], mine)
        for t in range(5):
            a_outs[i][0, 160 + 8 * (t // 4) : 168 + 8 * (t // 4), 128 * (t % 4) : 128 * (t % 4) + 128] = mine[
                8 * t : 8 * t + 8
            ].astype(BF)
    back = lax.dot_general(gate_grad, wg, nt, preferred_element_type=F32)
    back = back + lax.dot_general(up_grad, wu, nt, preferred_element_type=F32)
    for i in range(4):
        for j in range(4):
            at = (4 * i + j) * CAP
            a_outs[i][0, CAP * j : CAP * j + CAP, :] = back[at : at + CAP, 0:512].astype(BF)
            b_outs[j][0, i] = back[at : at + CAP, 512:1024].astype(BF)


def experts(xs, gs, w_gate, w_up, w_down, half):
    rows = pl.BlockSpec((1, 160, 1024), lambda e: (e, 0, 0))
    w_in = pl.BlockSpec((1, 1024, 384), lambda e: (2 * half + e, 0, 0))
    w_out = pl.BlockSpec((1, 384, 1024), lambda e: (2 * half + e, 0, 0))
    flat = [a.reshape(2, 160, 1024) for a in (*xs, *gs)]
    outs = pl.pallas_call(
        expert_body,
        out_shape=(jax.ShapeDtypeStruct((2, 176, 512), BF),) * 4 + (jax.ShapeDtypeStruct((2, SIDE, CAP, 512), BF),) * 4,
        grid=(2,),
        in_specs=[rows] * 8 + [w_in, w_in, w_out],
        out_specs=[pl.BlockSpec((1, 176, 512), lambda e: (e, 0, 0))] * 4
        + [pl.BlockSpec((1, SIDE, CAP, 512), lambda e: (e, 0, 0, 0))] * 4,
        compiler_params=pltpu.CompilerParams(vmem_limit_bytes=56 * 1024 * 1024),
        name="experts",
    )(*flat, w_gate, w_up, w_down)
    return outs[0:4], outs[4:8]


def combine_body(*refs):
    spreads_in, rows_in, outs = refs[0:2], refs[2:18], refs[18:26]
    weights, rows, stage, weight_sems, row_sems, out_sems = refs[26:]

    def loads(c, j):
        at = 4 * c + j
        yield pltpu.make_async_copy(spreads_in[c].at[j], weights.at[at], weight_sems.at[at])
        for n in range(8):
            source = rows_in[8 * c + n]
            part = source.at[:, CAP * j : CAP * j + CAP] if c == 0 else source.at[:, j]
            yield pltpu.make_async_copy(part, rows.at[at, n], row_sems.at[8 * at + n])

    order = [(c, j) for j in ORDER_LAST_OWN for c in range(2)]
    for c, j in order:
        for load in loads(c, j):
            load.start()
    stores = []
    for c, j in order:
        for load in loads(c, j):
            load.wait()
        at = 4 * c + j
        pieces = [rows[at, n, e].astype(F32) for n in range(8) for e in range(2)]
        joined = jnp.concatenate(pieces, axis=0).astype(BF)
        stage[at] = jnp.dot(weights[at], joined, preferred_element_type=F32).astype(BF)
        store = pltpu.make_async_copy(stage.at[at], outs[at], out_sems.at[at])
        store.start()
        stores.append(store)
    for store in stores:
        store.wait()


ORDER_LAST_OWN = (1, 3, 2, 0)


def combine(spread_a, spread_b, lows, highs):
    both = [pair[half][i] for pair in (lows, highs) for i in range(4) for half in range(2)]
    anywhere = pl.BlockSpec(memory_space=pl.ANY)
    outs = pl.pallas_call(
        combine_body,
        out_shape=(jax.ShapeDtypeStruct((256, 512), BF),) * 8,
        in_specs=[anywhere] * 18,
        out_specs=[anywhere] * 8,
        scratch_shapes=[
            pltpu.VMEM((8, 256, 16 * CAP), BF),
            pltpu.VMEM((8, 8, 2, CAP, 512), BF),
            pltpu.VMEM((8, 256, 512), BF),
            pltpu.SemaphoreType.DMA((8,)),
            pltpu.SemaphoreType.DMA((64,)),
            pltpu.SemaphoreType.DMA((8,)),
        ],
        name="combine",
    )(spread_a, spread_b, *both)
    return outs[0:4], outs[4:8]


def gather_probs_body(dest_ref, *refs):
    metas, low, high, outs = refs[0:4], refs[4:8], refs[8:12], refs[12:16]
    slot = iota((CAP, 256), 0).astype(F32)
    expert = expert_of_row(dest_ref, 16, 4, 0, 0)
    ranks = slot_ranks([m[:, 0:256].astype(F32) for m in metas], expert, 16)
    found = [[] for _ in range(4)]
    for i in range(4):
        for e in range(4):
            source = low[i] if e < 2 else high[i]
            for j in range(4):
                total = jnp.zeros((1, 256), F32)
                for t in range(5):
                    column = source[e % 2, 8 * (t // 4) : 8 * (t // 4) + 8, 128 * (t % 4) : 128 * (t % 4) + 128]
                    column = column.astype(F32)[:, j : j + 1]
                    hit = ranks[j][4 * i + e : 4 * i + e + 1] == slot[8 * t : 8 * t + 8]
                    total = total + jnp.sum(jnp.where(hit, column, 0.0), axis=0, keepdims=True)
                found[j].append(total)
    for j in range(4):
        outs[j][...] = jnp.concatenate(found[j], axis=0).astype(BF)


def gather_probs(dest, blocks, low, high):
    tail = pl.BlockSpec((2, 16, 512), lambda g, d: (0, 10, 0))
    return pl.pallas_call(
        gather_probs_body,
        out_shape=(jax.ShapeDtypeStruct((16, 256), BF),) * 4,
        grid_spec=pltpu.PrefetchScalarGridSpec(
            num_scalar_prefetch=1,
            grid=(1,),
            in_specs=[pl.BlockSpec((8, 1024), lambda g, d: (32, 0))] * 4 + [tail] * 8,
            out_specs=[pl.BlockSpec((16, 256), lambda g, d: (0, 0))] * 4,
        ),
        name="gather_probs",
    )(dest, *blocks, *low, *high)


def pick_probs_body(place_ref, meta, *refs):
    tables, prob_ref = refs[0:4], refs[4]
    ids = meta[:, 0:256].astype(F32)
    found = [jnp.zeros((16, 256), F32) for _ in range(8)]
    for j in range(4):
        expert = expert_of_row(place_ref, 16, 4, 0, 4 * j)
        values = tables[j][...].astype(F32)
        for k in range(8):
            found[k] = found[k] + jnp.where(ids[k : k + 1, :] == expert, values, 0.0)
    rows = [jnp.sum(f, axis=0, keepdims=True) for f in found]
    prob_ref[...] = jnp.concatenate(rows, axis=0).astype(BF)


def pick_probs(places, block, tables):
    return pl.pallas_call(
        pick_probs_body,
        out_shape=jax.ShapeDtypeStruct((8, 256), BF),
        grid_spec=pltpu.PrefetchScalarGridSpec(
            num_scalar_prefetch=1,
            grid=(1,),
            in_specs=[pl.BlockSpec((8, 1024), lambda g, d: (32, 0))]
            + [pl.BlockSpec((16, 256), lambda g, d: (0, 0))] * 4,
            out_specs=pl.BlockSpec((8, 256), lambda g, d: (0, 0)),
        ),
        name="pick_probs",
    )(places, block, *tables)


def finish_body(*refs):
    left, right, out_ref = refs[0:4], refs[4:8], refs[8]
    for at, parts in ((0, left), (512, right)):
        total = parts[0][...].astype(F32)
        for part in parts[1:]:
            total = total + part[...].astype(F32)
        out_ref[0, :, at : at + 512] = total.astype(BF)


def finish(left, right):
    return pl.pallas_call(
        finish_body, out_shape=jax.ShapeDtypeStruct((1, 256, 1024), BF), name="finish"
    )(*left, *right)


def weight_grad(masked, grads):
    return jnp.einsum("esd,esf->edf", masked, grads, preferred_element_type=F32).astype(BF)


ORDER = (1, 3, 2)


def spread_out(arrays, pairs_of, sign=1):
    out = {0: arrays[0]}
    for k in ORDER:
        out[k] = moved(arrays[k], pairs_of(sign * k))
    return [out[k] for k in range(4)]


def per_device(
    output_grad,
    layer_input,
    expert_ids,
    route_probs,
    gate_weight,
    up_weight,
    down_weight,
    saved_inputs,
    saved_gate_grad,
    saved_up_grad,
    saved_counts,
):
    here = lax.axis_index("ep").astype(jnp.int32)
    sections = lax.axis_size("section")
    y, z = here // 4, here % 4
    steps = jnp.arange(4, dtype=jnp.int32)
    column = 4 * ((y + steps) % 4) + z
    row = 4 * y + (z + steps) % 4
    dest = jnp.concatenate([column, row])
    places = (4 * ((y + steps) % 4)[None, :] + ((z + steps) % 4)[:, None]).reshape(16)
    w_gate, w_up, w_down = gate_weight[0], up_weight[0], down_weight[0]

    meta = jnp.concatenate(
        [expert_ids[0].T.astype(BF), route_probs[0].T, jnp.zeros((8, 512), BF)], axis=1
    )
    block_a = jnp.concatenate([layer_input[0], meta], axis=0)
    block_b = jnp.concatenate([output_grad[0], meta], axis=0)
    blocks_a = spread_out([block_a] * 4, along_z)
    blocks_b = spread_out([block_b] * 4, along_y)

    live = jnp.arange(CAP, dtype=jnp.int32)[None, None, :] < saved_counts[0][:, :, None]
    masked = saved_inputs[0] * live.reshape(saved_inputs.shape[1:3]).astype(BF)[:, :, None]
    gate_part = weight_grad(masked, saved_gate_grad[0])
    up_part = weight_grad(masked, saved_up_grad[0])

    lows, highs = [], []
    for half in range(2):
        sent_a, sent_b = select(dest, blocks_a, blocks_b, 2 * half)
        xs = spread_out(sent_a, along_y)
        gs = spread_out(sent_b, along_z)
        back_a, back_b = experts(xs, gs, w_gate, w_up, w_down, half)
        lows.append(spread_out(back_a, along_y, -1))
        highs.append(spread_out(back_b, along_z, -1))
    spread_a, spread_b = spreads(dest, blocks_a, blocks_b)
    made_a, made_b = combine(spread_a, spread_b, lows, highs)
    left = spread_out(made_a, along_z, -1)
    right = spread_out(made_b, along_y, -1)
    tables = gather_probs(dest, blocks_a, lows[0], lows[1])
    tables = spread_out(tables, along_z, -1)
    input_grad = finish(left, right)
    upstream = lax.ppermute(input_grad, "section", [(s, s - 1) for s in range(1, sections)])
    prob_rows = pick_probs(places, block_a, tables)
    return (upstream, prob_rows.T[None], gate_part[None], up_part[None])


def solution(mesh):
    rows = P("section", "ep", None)
    stacks = P("section", "ep", None, None)

    return jax.shard_map(
        per_device,
        mesh=mesh,
        in_specs=(rows, rows, rows, rows) + (stacks,) * 6 + (rows,),
        out_specs=(rows, rows, stacks, stacks),
        check_vma=False,
    )
```

```python
import functools

import jax
import jax.numpy as jnp
from jax import lax
from jax.experimental import pallas as pl
from jax.experimental.pallas import tpu as pltpu
from jax.sharding import PartitionSpec as P


BF = jnp.bfloat16
F32 = jnp.float32
SIDE = 4
CAP = 40


def along_z(k):
    return [(4 * y + z, 4 * y + (z + k) % 4) for y in range(4) for z in range(4)]


def along_y(k):
    return [(4 * y + z, 4 * ((y + k) % 4) + z) for y in range(4) for z in range(4)]


def in_vmem(arrays):
    return [pltpu.with_memory_space_constraint(a, pltpu.VMEM) for a in arrays]


def in_hbm(arrays):
    return [pltpu.with_memory_space_constraint(a, pltpu.HBM) for a in arrays]


VMEM_SPEC = pl.BlockSpec(memory_space=pltpu.VMEM)
SMEM_SPEC = pl.BlockSpec(memory_space=pltpu.SMEM)


def room(mib):
    return pltpu.CompilerParams(vmem_limit_bytes=mib * 1024 * 1024)


def moved(array, pairs):
    return lax.ppermute(array, "ep", pairs)


def iota(shape, dim):
    return lax.broadcasted_iota(jnp.int32, shape, dim)


def expert_of_row(dest_ref, rows, per_dest, first, base):
    row = iota((rows, 256), 0)
    expert = jnp.zeros((rows, 256), jnp.int32)
    for i in range(SIDE):
        expert = jnp.where(row // per_dest == i, 4 * dest_ref[base + i] + first + row % per_dest, expert)
    return expert.astype(F32)


def earlier():
    return (iota((256, 256), 0) < iota((256, 256), 1)).astype(BF)


def slot_ranks(ids_list, expert, rows):
    marks = []
    for ids in ids_list:
        mark = jnp.zeros((rows, 256), F32)
        for k in range(8):
            mark = mark + jnp.where(ids[k : k + 1, :] == expert, 1.0, 0.0)
        marks.append(mark)
    mark = jnp.concatenate(marks, axis=0)
    rank = jnp.dot(mark.astype(BF), earlier(), preferred_element_type=F32)
    rank = jnp.where(mark > 0.0, rank, -1.0)
    return [rank[rows * j : rows * j + rows] for j in range(len(ids_list))]


def select_own_body(dest_ref, *refs):
    blocks, outs = refs[:2], refs[2:10]
    slot = iota((16, CAP, 256), 1).astype(F32)
    for c in range(2):
        expert = expert_of_row(dest_ref, 16, 4, 0, 4 * c)
        mine = slot_ranks([blocks[c][256:264, 0:256].astype(F32)], expert, 16)[0]
        pick = jnp.where(mine[:, None, :] == slot, 1.0, 0.0).reshape(16 * CAP, 256).astype(BF)
        rows = jnp.dot(pick, blocks[c][0:256, :], preferred_element_type=F32)
        for i in range(SIDE):
            for e in range(4):
                at = (4 * i + e) * CAP
                outs[4 * c + i][e] = rows[at : at + CAP].astype(BF)


def select_own(dest, block_a, block_b):
    outs = pl.pallas_call(
        select_own_body,
        out_shape=(pltpu.VMEM((4, CAP, 1024), BF),) * 8,
        in_specs=[SMEM_SPEC] + [VMEM_SPEC] * 2,
        out_specs=[VMEM_SPEC] * 8,
        compiler_params=room(12),
        name="select_own",
    )(dest, *in_vmem([block_a, block_b]))
    return outs[:4], outs[4:]


def select_body(dest_ref, *refs, first):
    blocks, outs = refs[:6], refs[6:14]
    slot = iota((8, CAP, 256), 1).astype(F32)
    ranks = []
    for c in range(2):
        ids_list = [blocks[3 * c + j][256:264, 0:256].astype(F32) for j in range(3)]
        ranks.append(slot_ranks(ids_list, expert_of_row(dest_ref, 8, 2, first, 4 * c), 8))
    for j in range(3):
        for c in range(2):
            pick = jnp.where(ranks[c][j][:, None, :] == slot, 1.0, 0.0)
            pick = pick.reshape(8 * CAP, 256).astype(BF)
            rows = jnp.dot(pick, blocks[3 * c + j][0:256, :], preferred_element_type=F32)
            for i in range(SIDE):
                for e in range(2):
                    at = (2 * i + e) * CAP
                    outs[4 * c + i][e, j] = rows[at : at + CAP].astype(BF)


def select(dest, blocks_a, blocks_b, first):
    outs = pl.pallas_call(
        functools.partial(select_body, first=first),
        out_shape=(pltpu.VMEM((2, 3, CAP, 1024), BF),) * 8,
        in_specs=[SMEM_SPEC] + [VMEM_SPEC] * 6,
        out_specs=[VMEM_SPEC] * 8,
        compiler_params=room(10),
        name="select",
    )(dest, *in_vmem(blocks_a[1:] + blocks_b[1:]))
    return outs[:4], outs[4:]


def spread_body(dest_ref, *refs):
    metas, outs, rank_ref = refs[:8], refs[8:10], refs[10]
    slot = iota((16, CAP, 256), 1).astype(F32)
    for c in range(2):
        expert = expert_of_row(dest_ref, 16, 4, 0, 4 * c)
        mine = metas[4 * c : 4 * c + 4]
        ids_list = [m[256:264, 0:256].astype(F32) for m in mine]
        ranks = slot_ranks(ids_list, expert, 16)
        for j in range(4):
            weight = mine[j][256:264, 256:512].astype(F32)
            scale = jnp.zeros((16, 256), F32)
            for k in range(8):
                scale = scale + jnp.where(ids_list[j][k : k + 1, :] == expert, weight[k : k + 1, :], 0.0)
            spread = jnp.where(ranks[j][:, None, :] == slot, scale[:, None, :], 0.0).reshape(16 * CAP, 256)
            outs[c][j] = spread.T.astype(BF)
            if c == 0:
                rank_ref[j] = ranks[j]


def spreads(dest, blocks_a, blocks_b):
    return pl.pallas_call(
        spread_body,
        out_shape=(pltpu.VMEM((SIDE, 256, 16 * CAP), BF),) * 2 + (pltpu.VMEM((SIDE, 16, 256), F32),),
        in_specs=[SMEM_SPEC] + [VMEM_SPEC] * 8,
        out_specs=[VMEM_SPEC] * 3,
        compiler_params=room(10),
        name="spreads",
    )(dest, *in_vmem(blocks_a + blocks_b))


def expert_body(*refs, half):
    own_xs, xs, own_gs, gs = (refs[4 * k : 4 * k + 4] for k in range(4))
    wg_ref, wu_ref, wd_ref = refs[16:19]
    a_outs, b_outs = refs[-8:-4], refs[-4:]
    e = pl.program_id(0)

    def joined(own, others):
        pieces = [r.astype(F32) for a, b in zip(own, others) for r in (a[2 * half + e], b[e])]
        return jnp.concatenate(pieces, axis=0).astype(BF)

    rows, grads = joined(own_xs, xs), joined(own_gs, gs)
    wg, wu, wd = wg_ref[0], wu_ref[0], wd_ref[0]
    nt = (((1,), (1,)), ((), ()))
    gate = jnp.dot(rows, wg, preferred_element_type=F32)
    up = jnp.dot(rows, wu, preferred_element_type=F32)
    hg = lax.dot_general(grads, wd, nt, preferred_element_type=F32)
    hg = jnp.concatenate(
        [hg[(4 * j + i) * CAP : (4 * j + i + 1) * CAP] for i in range(4) for j in range(4)], axis=0
    )
    sigma = jax.nn.sigmoid(gate)
    active = gate * sigma
    hidden = (active * up).astype(BF).astype(F32)
    prob = jnp.sum(hidden * hg, axis=1, keepdims=True)
    gate_grad = (hg * up * sigma * (1.0 + gate * (1.0 - sigma))).astype(BF)
    up_grad = (hg * active).astype(BF)
    lane = iota((CAP, 128), 1)
    for i in range(4):
        mine = jnp.zeros((CAP, 128), F32)
        for j in range(4):
            at = (4 * i + j) * CAP
            mine = jnp.where(lane == j, prob[at : at + CAP], mine)
        for t in range(5):
            a_outs[i][e, 160 + 8 * (t // 4) : 168 + 8 * (t // 4), 128 * (t % 4) : 128 * (t % 4) + 128] = mine[
                8 * t : 8 * t + 8
            ].astype(BF)
    back = lax.dot_general(gate_grad, wg, nt, preferred_element_type=F32)
    back = back + lax.dot_general(up_grad, wu, nt, preferred_element_type=F32)
    for i in range(4):
        for j in range(4):
            at = (4 * i + j) * CAP
            a_outs[i][e, CAP * j : CAP * j + CAP, :] = back[at : at + CAP, 0:512].astype(BF)
            b_outs[j][e, i] = back[at : at + CAP, 512:1024].astype(BF)


def experts(own_xs, xs, own_gs, gs, w_gate, w_up, w_down, half):
    w_in = pl.BlockSpec((1, 1024, 384), lambda e: (2 * half + e, 0, 0))
    w_out = pl.BlockSpec((1, 384, 1024), lambda e: (2 * half + e, 0, 0))
    xs, gs = ([a.reshape(2, 120, 1024) for a in part] for part in (xs, gs))
    outs = pl.pallas_call(
        functools.partial(expert_body, half=half),
        out_shape=(pltpu.VMEM((2, 176, 512), BF),) * 4 + (pltpu.VMEM((2, SIDE, CAP, 512), BF),) * 4,
        grid=(2,),
        in_specs=[VMEM_SPEC] * 16 + [w_in, w_in, w_out],
        out_specs=[VMEM_SPEC] * 8,
        compiler_params=room(28),
        name="experts",
    )(*in_vmem([*own_xs, *xs, *own_gs, *gs]), w_gate, w_up, w_down)
    return outs[0:4], outs[4:8]


def values_at_tokens(rank, columns, j):
    slot = iota((CAP, 256), 0).astype(F32)
    found = []
    for r in range(16):
        one = jnp.where(rank[r : r + 1] == slot, columns[r][:, j : j + 1], 0.0)
        found.append(jnp.sum(one, axis=0, keepdims=True))
    return jnp.concatenate(found, axis=0)


def combine_body(*refs):
    rank_ref, weights, rows_in, outs = refs[0], refs[1:3], refs[3:19], refs[19:27]
    columns = []
    for source in rows_in[0:8]:
        for e in range(2):
            tile = [
                source[e, 160 + 8 * (t // 4) : 168 + 8 * (t // 4), 128 * (t % 4) : 128 * (t % 4) + 128]
                for t in range(5)
            ]
            columns.append(jnp.concatenate([t.astype(F32) for t in tile], axis=0))
    for j in range(4):
        for c in range(2):
            pieces = []
            for source in rows_in[8 * c : 8 * c + 8]:
                for e in range(2):
                    pieces.append(source[e, CAP * j : CAP * j + CAP] if c == 0 else source[e, j])
            joined = jnp.concatenate([p.astype(F32) for p in pieces], axis=0).astype(BF)
            out = outs[4 * c + j]
            out[0:256, :] = jnp.dot(weights[c][j], joined, preferred_element_type=F32).astype(BF)
            if c == 0:
                values = values_at_tokens(rank_ref[j], columns, j)
                out[256:264, 0:256] = values[0:8].astype(BF)
                out[256:264, 256:512] = values[8:16].astype(BF)


def combine(ranks, spread_a, spread_b, lows, highs):
    both = [pair[half][i] for pair in (lows, highs) for i in range(4) for half in range(2)]
    outs = pl.pallas_call(
        combine_body,
        out_shape=(pltpu.VMEM((264, 512), BF),) * 4 + (pltpu.VMEM((256, 512), BF),) * 4,
        in_specs=[VMEM_SPEC] * 19,
        out_specs=[VMEM_SPEC] * 8,
        compiler_params=room(12),
        name="combine",
    )(*in_vmem([ranks, spread_a, spread_b, *both]))
    return outs[0:4], outs[4:8]


def pick_probs_body(place_ref, meta, *refs):
    tables, prob_ref = refs[0:4], refs[4]
    ids = meta[256:264, 0:256].astype(F32)
    found = [jnp.zeros((8, 256), F32) for _ in range(8)]
    row = iota((8, 256), 0)
    for j in range(4):
        for part in range(2):
            values = tables[j][256:264, 256 * part : 256 * part + 256].astype(F32)
            at = 4 * j + 2 * part
            device = jnp.where(row // 4 == 0, place_ref[at], place_ref[at + 1])
            expert = (4 * device + row % 4).astype(F32)
            for k in range(8):
                found[k] = found[k] + jnp.where(ids[k : k + 1, :] == expert, values, 0.0)
    rows = [jnp.sum(f, axis=0, keepdims=True) for f in found]
    prob_ref[...] = jnp.concatenate(rows, axis=0).astype(BF)


def pick_probs(places, block, tables):
    return pl.pallas_call(
        pick_probs_body,
        out_shape=jax.ShapeDtypeStruct((8, 256), BF),
        in_specs=[SMEM_SPEC] + [VMEM_SPEC] * 5,
        compiler_params=room(4),
        name="pick_probs",
    )(places, *in_vmem([block, *tables]))


def finish_body(*refs):
    left, right, out_ref = refs[0:4], refs[4:8], refs[8]
    for at, parts in ((0, left), (512, right)):
        total = parts[0][0:256, :].astype(F32)
        for part in parts[1:]:
            total = total + part[0:256, :].astype(F32)
        out_ref[0, :, at : at + 512] = total.astype(BF)


def finish(left, right):
    return pl.pallas_call(
        finish_body,
        out_shape=pltpu.VMEM((1, 256, 1024), BF),
        in_specs=[VMEM_SPEC] * 8,
        out_specs=VMEM_SPEC,
        compiler_params=room(6),
        name="finish",
    )(*in_vmem(left), *in_vmem(right))


def weight_grads_body(count_ref, x_ref, gate_ref, up_ref, *refs, first):
    gate_out, up_out = refs[-2:]
    e = first + pl.program_id(0)
    slot = iota((CAP, 384), 0)
    gate, up = [], []
    for source in range(16):
        live = slot < count_ref[16 * e + source]
        at = CAP * source
        gate.append(jnp.where(live, gate_ref[0, at : at + CAP].astype(F32), 0.0))
        up.append(jnp.where(live, up_ref[0, at : at + CAP].astype(F32), 0.0))
    tn = (((0,), (0,)), ((), ()))
    for out, parts in ((gate_out, gate), (up_out, up)):
        grads = jnp.concatenate(parts, axis=0).astype(BF)
        out[0] = lax.dot_general(x_ref[0], grads, tn, preferred_element_type=F32).astype(BF)


def weight_grads(counts, inputs, gate, up, first, before=()):
    out = jax.ShapeDtypeStruct((4, 1024, 384), BF)
    anywhere = pl.BlockSpec(memory_space=pl.ANY)
    return pl.pallas_call(
        functools.partial(weight_grads_body, first=first),
        out_shape=(out, out),
        grid_spec=pltpu.PrefetchScalarGridSpec(
            num_scalar_prefetch=1,
            grid=(2,),
            in_specs=[pl.BlockSpec((1, 640, 1024), lambda g, c: (first + g, 0, 0))]
            + [pl.BlockSpec((1, 640, 384), lambda g, c: (first + g, 0, 0))] * 2
            + [anywhere] * len(before),
            out_specs=[pl.BlockSpec((1, 1024, 384), lambda g, c: (first + g, 0, 0))] * 2,
        ),
        input_output_aliases={4: 0, 5: 1} if before else {},
        compiler_params=room(20),
        name="weight_grads",
    )(counts, *in_hbm([inputs, gate, up]), *before)


ORDER = (2, 1, 3)


def spread_out(arrays, pairs_of, sign=1):
    out = {0: arrays[0]}
    for k in ORDER:
        out[k] = moved(arrays[k], pairs_of(sign * k))
    return [out[k] for k in range(4)]


def per_device(
    output_grad,
    layer_input,
    expert_ids,
    route_probs,
    gate_weight,
    up_weight,
    down_weight,
    saved_inputs,
    saved_gate_grad,
    saved_up_grad,
    saved_counts,
):
    here = lax.axis_index("ep").astype(jnp.int32)
    sections = lax.axis_size("section")
    y, z = here // 4, here % 4
    steps = jnp.arange(4, dtype=jnp.int32)
    column = 4 * ((y + steps) % 4) + z
    row = 4 * y + (z + steps) % 4
    dest = jnp.concatenate([column, row])
    places = (4 * ((y + steps) % 4)[None, :] + ((z + steps) % 4)[:, None]).reshape(16)
    w_gate, w_up, w_down = gate_weight[0], up_weight[0], down_weight[0]

    meta = jnp.concatenate(
        [expert_ids[0].T.astype(BF), route_probs[0].T, jnp.zeros((8, 512), BF)], axis=1
    )
    block_a = jnp.concatenate([layer_input[0], meta], axis=0)
    block_b = jnp.concatenate([output_grad[0], meta], axis=0)
    blocks_a = spread_out([block_a] * 4, along_z)
    blocks_b = spread_out([block_b] * 4, along_y)

    saved = (saved_counts[0].reshape(-1), saved_inputs[0], saved_gate_grad[0], saved_up_grad[0])
    partly = weight_grads(*saved, 0)
    gate_part, up_part = weight_grads(*saved, 2, partly)

    sent_a, sent_b = select_own(dest, block_a, block_b)
    own_xs = spread_out(sent_a, along_y)
    own_gs = spread_out(sent_b, along_z)
    lows, highs = [], []
    for half in range(2):
        sent_a, sent_b = select(dest, blocks_a, blocks_b, 2 * half)
        xs = spread_out(sent_a, along_y)
        gs = spread_out(sent_b, along_z)
        back_a, back_b = experts(own_xs, xs, own_gs, gs, w_gate, w_up, w_down, half)
        lows.append(spread_out(back_a, along_y, -1))
        highs.append(spread_out(back_b, along_z, -1))
    spread_a, spread_b, ranks = spreads(dest, blocks_a, blocks_b)
    made_a, made_b = combine(ranks, spread_a, spread_b, lows, highs)
    left = spread_out(made_a, along_z, -1)
    right = spread_out(made_b, along_y, -1)
    input_grad = finish(left, right)
    upstream = lax.ppermute(input_grad, "section", [(s, s - 1) for s in range(1, sections)])
    prob_rows = pick_probs(places, block_a, left)
    return (upstream, prob_rows.T[None], gate_part[None], up_part[None])


def solution(mesh):
    rows = P("section", "ep", None)
    stacks = P("section", "ep", None, None)

    return jax.shard_map(
        per_device,
        mesh=mesh,
        in_specs=(rows, rows, rows, rows) + (stacks,) * 6 + (rows,),
        out_specs=(rows, rows, stacks, stacks),
        check_vma=False,
    )
```

```python
import functools

import jax
import jax.numpy as jnp
from jax import lax
from jax.experimental import pallas as pl
from jax.experimental.pallas import tpu as pltpu
from jax.sharding import PartitionSpec as P


BF = jnp.bfloat16
F32 = jnp.float32
SIDE = 4
CAP = 40


def along_z(k):
    return [(4 * y + z, 4 * y + (z + k) % 4) for y in range(4) for z in range(4)]


def along_y(k):
    return [(4 * y + z, 4 * ((y + k) % 4) + z) for y in range(4) for z in range(4)]


def in_vmem(arrays):
    return [pltpu.with_memory_space_constraint(a, pltpu.VMEM) for a in arrays]


def in_hbm(arrays):
    return [pltpu.with_memory_space_constraint(a, pltpu.HBM) for a in arrays]


VMEM_SPEC = pl.BlockSpec(memory_space=pltpu.VMEM)
SMEM_SPEC = pl.BlockSpec(memory_space=pltpu.SMEM)


def room(mib):
    return pltpu.CompilerParams(vmem_limit_bytes=mib * 1024 * 1024)


def moved(array, pairs):
    return lax.ppermute(array, "ep", pairs)


def iota(shape, dim):
    return lax.broadcasted_iota(jnp.int32, shape, dim)


def expert_of_row(dest_ref, rows, per_dest, first, base):
    row = iota((rows, 256), 0)
    expert = jnp.zeros((rows, 256), jnp.int32)
    for i in range(SIDE):
        expert = jnp.where(row // per_dest == i, 4 * dest_ref[base + i] + first + row % per_dest, expert)
    return expert.astype(F32)


def earlier():
    return (iota((256, 256), 0) < iota((256, 256), 1)).astype(BF)


def slot_ranks(ids_list, expert, rows):
    marks = []
    for ids in ids_list:
        mark = jnp.zeros((rows, 256), F32)
        for k in range(8):
            mark = mark + jnp.where(ids[k : k + 1, :] == expert, 1.0, 0.0)
        marks.append(mark)
    mark = jnp.concatenate(marks, axis=0)
    rank = jnp.dot(mark.astype(BF), earlier(), preferred_element_type=F32)
    rank = jnp.where(mark > 0.0, rank, -1.0)
    return [rank[rows * j : rows * j + rows] for j in range(len(ids_list))]


def select_own_body(dest_ref, *refs):
    blocks, outs = refs[:2], refs[2:10]
    slot = iota((16, CAP, 256), 1).astype(F32)
    for c in range(2):
        expert = expert_of_row(dest_ref, 16, 4, 0, 4 * c)
        mine = slot_ranks([blocks[c][256:264, 0:256].astype(F32)], expert, 16)[0]
        pick = jnp.where(mine[:, None, :] == slot, 1.0, 0.0).reshape(16 * CAP, 256).astype(BF)
        rows = jnp.dot(pick, blocks[c][0:256, :], preferred_element_type=F32)
        for i in range(SIDE):
            for e in range(4):
                at = (4 * i + e) * CAP
                outs[4 * c + i][e] = rows[at : at + CAP].astype(BF)


def select_own(dest, block_a, block_b):
    outs = pl.pallas_call(
        select_own_body,
        out_shape=(pltpu.VMEM((4, CAP, 1024), BF),) * 8,
        in_specs=[SMEM_SPEC] + [VMEM_SPEC] * 2,
        out_specs=[VMEM_SPEC] * 8,
        compiler_params=room(12),
        name="select_own",
    )(dest, *in_vmem([block_a, block_b]))
    return outs[:4], outs[4:]


def select_body(dest_ref, *refs, first):
    blocks, outs = refs[:6], refs[6:14]
    slot = iota((8, CAP, 256), 1).astype(F32)
    ranks = []
    for c in range(2):
        ids_list = [blocks[3 * c + j][256:264, 0:256].astype(F32) for j in range(3)]
        ranks.append(slot_ranks(ids_list, expert_of_row(dest_ref, 8, 2, first, 4 * c), 8))
    for j in range(3):
        for c in range(2):
            pick = jnp.where(ranks[c][j][:, None, :] == slot, 1.0, 0.0)
            pick = pick.reshape(8 * CAP, 256).astype(BF)
            rows = jnp.dot(pick, blocks[3 * c + j][0:256, :], preferred_element_type=F32)
            for i in range(SIDE):
                for e in range(2):
                    at = (2 * i + e) * CAP
                    outs[4 * c + i][e, j] = rows[at : at + CAP].astype(BF)


def select(dest, blocks_a, blocks_b, first):
    outs = pl.pallas_call(
        functools.partial(select_body, first=first),
        out_shape=(pltpu.VMEM((2, 3, CAP, 1024), BF),) * 8,
        in_specs=[SMEM_SPEC] + [VMEM_SPEC] * 6,
        out_specs=[VMEM_SPEC] * 8,
        compiler_params=room(10),
        name="select",
    )(dest, *in_vmem(blocks_a[1:] + blocks_b[1:]))
    return outs[:4], outs[4:]


def spread_body(dest_ref, *refs):
    metas, outs, rank_ref = refs[:8], refs[8:10], refs[10]
    slot = iota((16, CAP, 256), 1).astype(F32)
    for c in range(2):
        expert = expert_of_row(dest_ref, 16, 4, 0, 4 * c)
        mine = metas[4 * c : 4 * c + 4]
        ids_list = [m[256:264, 0:256].astype(F32) for m in mine]
        ranks = slot_ranks(ids_list, expert, 16)
        for j in range(4):
            weight = mine[j][256:264, 256:512].astype(F32)
            scale = jnp.zeros((16, 256), F32)
            for k in range(8):
                scale = scale + jnp.where(ids_list[j][k : k + 1, :] == expert, weight[k : k + 1, :], 0.0)
            spread = jnp.where(ranks[j][:, None, :] == slot, scale[:, None, :], 0.0).reshape(16 * CAP, 256)
            outs[c][j] = spread.T.astype(BF)
            if c == 0:
                rank_ref[j] = ranks[j]


def spreads(dest, blocks_a, blocks_b):
    return pl.pallas_call(
        spread_body,
        out_shape=(pltpu.VMEM((SIDE, 256, 16 * CAP), BF),) * 2 + (pltpu.VMEM((SIDE, 16, 256), F32),),
        in_specs=[SMEM_SPEC] + [VMEM_SPEC] * 8,
        out_specs=[VMEM_SPEC] * 3,
        compiler_params=room(10),
        name="spreads",
    )(dest, *in_vmem(blocks_a + blocks_b))


def expert_body(*refs, half):
    own_xs, xs, own_gs, gs = (refs[4 * k : 4 * k + 4] for k in range(4))
    wg_ref, wu_ref, wd_ref = refs[16:19]
    a_outs, b_outs = refs[-8:-4], refs[-4:]
    e = pl.program_id(0)

    def joined(own, others):
        pieces = [r.astype(F32) for a, b in zip(own, others) for r in (a[2 * half + e], b[e])]
        return jnp.concatenate(pieces, axis=0).astype(BF)

    rows, grads = joined(own_xs, xs), joined(own_gs, gs)
    wg, wu, wd = wg_ref[0], wu_ref[0], wd_ref[0]
    nt = (((1,), (1,)), ((), ()))
    gate = jnp.dot(rows, wg, preferred_element_type=F32)
    up = jnp.dot(rows, wu, preferred_element_type=F32)
    hg = lax.dot_general(grads, wd, nt, preferred_element_type=F32)
    hg = jnp.concatenate(
        [hg[(4 * j + i) * CAP : (4 * j + i + 1) * CAP] for i in range(4) for j in range(4)], axis=0
    )
    sigma = jax.nn.sigmoid(gate)
    active = gate * sigma
    hidden = (active * up).astype(BF).astype(F32)
    prob = jnp.sum(hidden * hg, axis=1, keepdims=True)
    gate_grad = (hg * up * sigma * (1.0 + gate * (1.0 - sigma))).astype(BF)
    up_grad = (hg * active).astype(BF)
    lane = iota((8, 128), 1)
    for i in range(4):
        tiles = [jnp.zeros((8, 128), F32) for _ in range(4)]
        for t in range(5):
            for j in range(4):
                at = (4 * i + j) * CAP + 8 * t
                tiles[t % 4] = jnp.where(lane == j + 4 * (t // 4), prob[at : at + 8], tiles[t % 4])
        a_outs[i][e, 160:168, :] = jnp.concatenate(tiles, axis=1).astype(BF)
    back = lax.dot_general(gate_grad, wg, nt, preferred_element_type=F32)
    back = back + lax.dot_general(up_grad, wu, nt, preferred_element_type=F32)
    for i in range(4):
        for j in range(4):
            at = (4 * i + j) * CAP
            a_outs[i][e, CAP * j : CAP * j + CAP, :] = back[at : at + CAP, 0:512].astype(BF)
            b_outs[j][e, i] = back[at : at + CAP, 512:1024].astype(BF)


def experts(own_xs, xs, own_gs, gs, w_gate, w_up, w_down, half):
    w_in = pl.BlockSpec((1, 1024, 384), lambda e: (2 * half + e, 0, 0))
    w_out = pl.BlockSpec((1, 384, 1024), lambda e: (2 * half + e, 0, 0))
    xs, gs = ([a.reshape(2, 120, 1024) for a in part] for part in (xs, gs))
    outs = pl.pallas_call(
        functools.partial(expert_body, half=half),
        out_shape=(pltpu.VMEM((2, 168, 512), BF),) * 4 + (pltpu.VMEM((2, SIDE, CAP, 512), BF),) * 4,
        grid=(2,),
        in_specs=[VMEM_SPEC] * 16 + [w_in, w_in, w_out],
        out_specs=[VMEM_SPEC] * 8,
        compiler_params=room(28),
        name="experts",
    )(*in_vmem([*own_xs, *xs, *own_gs, *gs]), w_gate, w_up, w_down)
    return outs[0:4], outs[4:8]


def values_at_tokens(rank, tails, j):
    slot = iota((CAP, 256), 0).astype(F32)
    found = []
    for r in range(16):
        lanes = [128 * (t % 4) + j + 4 * (t // 4) for t in range(5)]
        column = jnp.concatenate([tails[r][:, n : n + 1] for n in lanes], axis=0)
        one = jnp.where(rank[r : r + 1] == slot, column, 0.0)
        found.append(jnp.sum(one, axis=0, keepdims=True))
    return jnp.concatenate(found, axis=0)


def combine_body(*refs, sources):
    rank_ref, weights, rows_in, outs = refs[0], refs[1:3], refs[3:19], refs[19:]
    tails = [source[e, 160:168, :].astype(F32) for source in rows_in[0:8] for e in range(2)]
    for at, j in enumerate(sources):
        for c in range(2):
            pieces = []
            for source in rows_in[8 * c : 8 * c + 8]:
                for e in range(2):
                    pieces.append(source[e, CAP * j : CAP * j + CAP] if c == 0 else source[e, j])
            joined = jnp.concatenate([p.astype(F32) for p in pieces], axis=0).astype(BF)
            out = outs[len(sources) * c + at]
            out[0:256, :] = jnp.dot(weights[c][j], joined, preferred_element_type=F32).astype(BF)
            if c == 0:
                values = values_at_tokens(rank_ref[j], tails, j)
                out[256:264, 0:256] = values[0:8].astype(BF)
                out[256:264, 256:512] = values[8:16].astype(BF)


def combine(ranks, spread_a, spread_b, lows, highs, sources):
    both = [pair[half][i] for pair in (lows, highs) for i in range(4) for half in range(2)]
    count = len(sources)
    outs = pl.pallas_call(
        functools.partial(combine_body, sources=sources),
        out_shape=(pltpu.VMEM((264, 512), BF),) * count + (pltpu.VMEM((256, 512), BF),) * count,
        in_specs=[VMEM_SPEC] * 19,
        out_specs=[VMEM_SPEC] * (2 * count),
        compiler_params=room(12),
        name="combine",
    )(*in_vmem([ranks, spread_a, spread_b, *both]))
    return dict(zip(sources, outs[:count])), dict(zip(sources, outs[count:]))


def pick_probs_body(place_ref, meta, *refs):
    tables, prob_ref = refs[0:4], refs[4]
    ids = meta[256:264, 0:256].astype(F32)
    found = [jnp.zeros((8, 256), F32) for _ in range(8)]
    row = iota((8, 256), 0)
    for j in range(4):
        for part in range(2):
            values = tables[j][256:264, 256 * part : 256 * part + 256].astype(F32)
            at = 4 * j + 2 * part
            device = jnp.where(row // 4 == 0, place_ref[at], place_ref[at + 1])
            expert = (4 * device + row % 4).astype(F32)
            for k in range(8):
                found[k] = found[k] + jnp.where(ids[k : k + 1, :] == expert, values, 0.0)
    rows = [jnp.sum(f, axis=0, keepdims=True) for f in found]
    prob_ref[...] = jnp.concatenate(rows, axis=0).astype(BF)


def pick_probs(places, block, tables):
    return pl.pallas_call(
        pick_probs_body,
        out_shape=jax.ShapeDtypeStruct((8, 256), BF),
        in_specs=[SMEM_SPEC] + [VMEM_SPEC] * 5,
        compiler_params=room(4),
        name="pick_probs",
    )(places, *in_vmem([block, *tables]))


def finish_body(*refs):
    left, right, out_ref = refs[0:4], refs[4:8], refs[8]
    for at, parts in ((0, left), (512, right)):
        total = parts[0][0:256, :].astype(F32)
        for part in parts[1:]:
            total = total + part[0:256, :].astype(F32)
        out_ref[0, :, at : at + 512] = total.astype(BF)


def finish(left, right):
    return pl.pallas_call(
        finish_body,
        out_shape=pltpu.VMEM((1, 256, 1024), BF),
        in_specs=[VMEM_SPEC] * 8,
        out_specs=VMEM_SPEC,
        compiler_params=room(6),
        name="finish",
    )(*in_vmem(left), *in_vmem(right))


def weight_grads_body(count_ref, x_ref, gate_ref, up_ref, *refs, first):
    gate_out, up_out = refs[-2:]
    e = first + pl.program_id(0)
    slot = iota((CAP, 384), 0)
    gate, up = [], []
    for source in range(16):
        live = slot < count_ref[16 * e + source]
        at = CAP * source
        gate.append(jnp.where(live, gate_ref[0, at : at + CAP].astype(F32), 0.0))
        up.append(jnp.where(live, up_ref[0, at : at + CAP].astype(F32), 0.0))
    tn = (((0,), (0,)), ((), ()))
    for out, parts in ((gate_out, gate), (up_out, up)):
        grads = jnp.concatenate(parts, axis=0).astype(BF)
        out[0] = lax.dot_general(x_ref[0], grads, tn, preferred_element_type=F32).astype(BF)


def weight_grads(counts, inputs, gate, up, first, before=()):
    out = jax.ShapeDtypeStruct((4, 1024, 384), BF)
    anywhere = pl.BlockSpec(memory_space=pl.ANY)
    return pl.pallas_call(
        functools.partial(weight_grads_body, first=first),
        out_shape=(out, out),
        grid_spec=pltpu.PrefetchScalarGridSpec(
            num_scalar_prefetch=1,
            grid=(2,),
            in_specs=[pl.BlockSpec((1, 640, 1024), lambda g, c: (first + g, 0, 0))]
            + [pl.BlockSpec((1, 640, 384), lambda g, c: (first + g, 0, 0))] * 2
            + [anywhere] * len(before),
            out_specs=[pl.BlockSpec((1, 1024, 384), lambda g, c: (first + g, 0, 0))] * 2,
        ),
        input_output_aliases={4: 0, 5: 1} if before else {},
        compiler_params=room(20),
        name="weight_grads",
    )(counts, *in_hbm([inputs, gate, up]), *before)


ORDER = (2, 1, 3)


def spread_out(arrays, pairs_of, sign=1):
    out = {0: arrays[0]}
    for k in ORDER:
        out[k] = moved(arrays[k], pairs_of(sign * k))
    return [out[k] for k in range(4)]


def per_device(
    output_grad,
    layer_input,
    expert_ids,
    route_probs,
    gate_weight,
    up_weight,
    down_weight,
    saved_inputs,
    saved_gate_grad,
    saved_up_grad,
    saved_counts,
):
    here = lax.axis_index("ep").astype(jnp.int32)
    sections = lax.axis_size("section")
    y, z = here // 4, here % 4
    steps = jnp.arange(4, dtype=jnp.int32)
    column = 4 * ((y + steps) % 4) + z
    row = 4 * y + (z + steps) % 4
    dest = jnp.concatenate([column, row])
    places = (4 * ((y + steps) % 4)[None, :] + ((z + steps) % 4)[:, None]).reshape(16)
    w_gate, w_up, w_down = gate_weight[0], up_weight[0], down_weight[0]

    meta = jnp.concatenate(
        [expert_ids[0].T.astype(BF), route_probs[0].T, jnp.zeros((8, 512), BF)], axis=1
    )
    block_a = jnp.concatenate([layer_input[0], meta], axis=0)
    block_b = jnp.concatenate([output_grad[0], meta], axis=0)
    blocks_a = spread_out([block_a] * 4, along_z)
    blocks_b = spread_out([block_b] * 4, along_y)

    saved = (saved_counts[0].reshape(-1), saved_inputs[0], saved_gate_grad[0], saved_up_grad[0])
    partly = weight_grads(*saved, 0)
    gate_part, up_part = weight_grads(*saved, 2, partly)

    sent_a, sent_b = select_own(dest, block_a, block_b)
    own_xs = spread_out(sent_a, along_y)
    own_gs = spread_out(sent_b, along_z)
    lows, highs = [], []
    for half in range(2):
        sent_a, sent_b = select(dest, blocks_a, blocks_b, 2 * half)
        xs = spread_out(sent_a, along_y)
        gs = spread_out(sent_b, along_z)
        back_a, back_b = experts(own_xs, xs, own_gs, gs, w_gate, w_up, w_down, half)
        lows.append(spread_out(back_a, along_y, -1))
        highs.append(spread_out(back_b, along_z, -1))
    spread_a, spread_b, ranks = spreads(dest, blocks_a, blocks_b)
    made_a, made_b = combine(ranks, spread_a, spread_b, lows, highs, (2,))
    more_a, more_b = combine(ranks, spread_a, spread_b, lows, highs, (1, 3, 0))
    made_a, made_b = {**made_a, **more_a}, {**made_b, **more_b}
    left = spread_out(made_a, along_z, -1)
    right = spread_out(made_b, along_y, -1)
    input_grad = finish(left, right)
    upstream = lax.ppermute(input_grad, "section", [(s, s - 1) for s in range(1, sections)])
    prob_rows = pick_probs(places, block_a, left)
    return (upstream, prob_rows.T[None], gate_part[None], up_part[None])


def solution(mesh):
    rows = P("section", "ep", None)
    stacks = P("section", "ep", None, None)

    return jax.shard_map(
        per_device,
        mesh=mesh,
        in_specs=(rows, rows, rows, rows) + (stacks,) * 6 + (rows,),
        out_specs=(rows, rows, stacks, stacks),
        check_vma=False,
    )
```
